8 devices in a mesh: dp: 1 (over z), c: 2 (over y), r: 4 (over x, core).
Axes of the slice: x: 2, y: 2, z: 1, core: 2. Of those that a mesh axis runs over, the one named last changes fastest.
Arguments:
- x: bfloat16 [4096, 2048], P(('dp', 'r'), 'c')
- w: bfloat16 [2048, 16384], P('r', 'c')
- dy: bfloat16 [4096, 16384], P(('dp', 'r'), 'c')
Outputs:
- output 1: bfloat16 [4096, 2048], P(('dp', 'r'), 'c')
- output 2: float32 [2048, 16384], P(('dp', 'r'), 'c')
All inputs are finite; a program needn't handle non-finite values.
Results may differ from the reference program's by a relative error of at most 0.001.
Values are sent between devices in bfloat16 or wider.
A program may use at most 1 GiB of HBM per device.

```python
import jax
import jax.numpy as jnp

T = 4096
H = 2048
F = 8192


def setup_inputs(seed: int = 0, part: int = 0) -> dict:
    base = jax.random.PRNGKey(seed)
    kw, kpart = jax.random.split(base)
    kx, kdy = jax.random.split(jax.random.fold_in(kpart, part))
    n = 2 * F
    x = jax.random.normal(kx, (T, H), jnp.float32)
    w = jax.random.normal(kw, (H, n), jnp.float32) * H ** -0.5
    dy = jax.random.normal(kdy, (T, n), jnp.float32) * (T * n / H) ** -0.25
    return {"x": x.astype(jnp.bfloat16), "w": w.astype(jnp.bfloat16), "dy": dy.astype(jnp.bfloat16)}


def reference(x, w, dy):
    dx = jnp.dot(dy, w.T, preferred_element_type=jnp.float32).astype(jnp.bfloat16)
    dw = jnp.dot(x.T, dy, preferred_element_type=jnp.float32)
    return dx, dw
```

```python
import jax
import jax.numpy as jnp
from jax import lax
from jax.experimental import pallas as pl
from jax.experimental.pallas import tpu as pltpu
from jax.sharding import PartitionSpec as P

MESH = pl.DeviceIdType.MESH
T = 64
TILE = 1024


def kernel(x, w, dy, dx, dw, far, far2, near, wv, xg, buf, xt, part, part_in, out,
           load_s, w_s, xl_s, xs_s, xr_s, xf_s, ys_s, yr_s, ns_s, nr_s, fs_s, fr_s,
           ps_s, pr_s, os_s, or_s, ol_s):
    rows, half = x.shape[0], x.shape[1] // 2
    cols = w.shape[1]
    steps = rows // T
    z, c, r = lax.axis_index("dp"), lax.axis_index("c"), lax.axis_index("r")
    chip, core = r // 2, r % 2
    far_chip = 1 - chip
    here = chip == c

    def device(cc, chip_, core_):
        return {"dp": z, "c": cc, "r": 2 * chip_ + core_}

    mate = device(c, chip, 1 - core)
    x_same, x_other = device(c, far_chip, core), device(c, far_chip, 1 - core)
    y_same, y_other = device(1 - c, chip, core), device(1 - c, chip, 1 - core)

    def remote(src, dst, send, recv, dev):
        return pltpu.make_async_remote_copy(src, dst, send, recv, device_id=dev,
                                            device_id_type=MESH)

    def x_block(t):
        return xg.at[pl.ds(pl.multiple_of(t * rows, rows), rows), :]

    def x_half(k):
        return x.at[:, pl.ds(pl.multiple_of(k * half, half), half)]

    def piece(ref, q):
        return ref.at[pl.ds(pl.multiple_of(q * T, T), T), :]

    barrier = pltpu.get_barrier_semaphore()
    peers = (mate, x_same, x_other, y_same, y_other)
    for p in peers:
        pl.semaphore_signal(barrier, inc=1, device_id=p, device_id_type=MESH)
    pl.semaphore_wait(barrier, len(peers))

    @pl.when(jnp.logical_not(here))
    def _():
        remote(x_half(core), x_block(r), xs_s.at[0], xr_s.at[r], x_same).start()
        remote(x_half(1 - core), x_block(r), xs_s.at[1], xr_s.at[r], x_other).start()

    @pl.when(here)
    def _():
        remote(x_half(core), x_block(r), xs_s.at[0], xr_s.at[r], y_same).start()
        remote(x_half(1 - core), x_block(r), xs_s.at[1], xr_s.at[r], y_other).start()
        remote(x_half(1 - core), x_block(r), xs_s.at[2], xr_s.at[r], mate).start()
        pltpu.make_async_copy(x_half(core), x_block(r), xl_s).start()

    @pl.loop(0, steps)
    def _(q):
        remote(piece(dy, q), piece(far, q), ys_s, yr_s.at[q], x_same).start()

    @pl.loop(0, steps)
    def _(q):
        remote(piece(dy, q), piece(near, q), ns_s, nr_s.at[q], mate).start()

    pltpu.make_async_copy(w, wv, w_s).start()

    @pl.loop(0, cols // TILE)
    def _(t):
        dw[:, pl.ds(pl.multiple_of(t * TILE, TILE), TILE)] = jnp.zeros((dw.shape[0], TILE), jnp.float32)

    pltpu.make_async_copy(w, wv, w_s).wait()

    mine, other = r, 2 * chip + 1 - core
    far_mine, far_other = 2 * far_chip + core, 2 * far_chip + 1 - core

    @pl.when(here)
    def _():
        pltpu.make_async_copy(x_half(core), x_block(r), xl_s).wait()

    @pl.when(jnp.logical_not(here))
    def _():
        remote(x_half(core), x_block(mine), xs_s.at[0], xr_s.at[mine], y_same).wait_recv()

    remote(x_half(core), x_block(other), xs_s.at[0], xr_s.at[other], y_same).wait_recv()

    def compute(slot, ta, tb, q):
        row = pl.multiple_of(q * T, T)
        xa = xg[pl.ds(pl.multiple_of(ta * rows + row, T), T), :]
        xb = xg[pl.ds(pl.multiple_of(tb * rows + row, T), T), :]
        xt[...] = jnp.concatenate([xa, xb], axis=0).T
        part[slot] = jnp.zeros(part.shape[1:], jnp.float32)

        @pl.loop(0, cols // TILE)
        def _(t):
            cs = pl.ds(pl.multiple_of(t * TILE, TILE), TILE)
            d = buf[:, cs]
            part[slot] += lax.dot_general(d, wv[:, cs], (((1,), (1,)), ((), ())),
                                          preferred_element_type=jnp.float32)
            dw[:, cs] += jnp.dot(xt[...], d, preferred_element_type=jnp.float32)

    def load(src, q, lo):
        return pltpu.make_async_copy(piece(src, q), buf.at[pl.ds(lo * T, T), :], load_s.at[lo])

    def send_part(slot):
        return remote(part.at[slot], part_in.at[slot], ps_s, pr_s.at[slot], y_same)

    @pl.loop(0, steps)
    def _(q):
        load(dy, q, 0).start()
        remote(piece(dy, q), piece(near, q), ns_s, nr_s.at[q], mate).wait_recv()
        load(near, q, 1).start()
        load(dy, q, 0).wait()
        load(near, q, 1).wait()
        compute(q, mine, other, q)

        @pl.when(jnp.logical_not(here))
        def _():
            send_part(q).start()

    for t in range(2):
        src_t = 2 * far_chip + t
        remote(x_half(core), x_block(src_t), xs_s.at[0], xr_s.at[src_t], x_same).wait_recv()

        @pl.when(here)
        def _():
            remote(x_block(src_t), x_block(src_t), xf_s.at[t], xr_s.at[src_t], y_same).start()

    def dx_piece(q):
        return dx.at[pl.ds(pl.multiple_of(q * T, T), T),
                     pl.ds(pl.multiple_of(core * half, half), half)]

    def finish(slot):
        send_part(slot).wait_recv()
        out[slot] = (part[slot] + part_in[slot]).astype(jnp.bfloat16)

    @pl.loop(0, steps)
    def _(q):
        slot = steps + q
        remote(piece(dy, q), piece(far, q), ys_s, yr_s.at[q], x_same).wait_recv()
        remote(piece(far, q), piece(far2, q), fs_s, fr_s.at[q], mate).start()
        load(far, q, 0).start()
        remote(piece(far, q), piece(far2, q), fs_s, fr_s.at[q], mate).wait_recv()
        load(far2, q, 1).start()
        load(far, q, 0).wait()
        load(far2, q, 1).wait()
        compute(slot, far_mine, far_other, q)

        @pl.when(jnp.logical_not(here))
        def _():
            send_part(slot).start()

        @pl.when(here)
        def _():
            finish(slot)
            remote(out.at[slot, pl.ds(0, T), :], dx_piece(q), os_s.at[0], or_s, x_same).start()
            remote(out.at[slot, pl.ds(T, T), :], dx_piece(q), os_s.at[1], or_s, x_other).start()
            finish(q)
            pltpu.make_async_copy(out.at[q, pl.ds(0, T), :], dx_piece(q), ol_s).start()
            remote(out.at[q, pl.ds(T, T), :], dx_piece(q), os_s.at[2], or_s, mate).start()

    remote(dy, far, ys_s, yr_s.at[0], x_same).wait_send()
    remote(dy, near, ns_s, nr_s.at[0], mate).wait_send()
    remote(far, far2, fs_s, fr_s.at[0], mate).wait_send()
    for t in range(2):
        remote(x_half(core), x_block(r), xs_s.at[t], xr_s.at[r], x_same).wait_send()

    @pl.when(jnp.logical_not(here))
    def _():
        remote(part, part_in, ps_s, pr_s.at[0], y_same).wait_send()
        remote(dx, dx, os_s.at[0], or_s, x_same).wait_recv()

    @pl.when(here)
    def _():
        remote(x_half(core), x_block(r), xs_s.at[2], xr_s.at[r], mate).wait_send()
        for t in range(2):
            remote(x_block(t), x_block(t), xf_s.at[t], xr_s.at[r], y_same).wait_send()
        dx_half = dx.at[:, pl.ds(0, half)]
        for t in range(3):
            remote(dx_half, dx_half, os_s.at[t], or_s, mate).wait_send()
        pltpu.make_async_copy(dx_half, dx_half, ol_s).wait()
        remote(dx_half, dx_half, os_s.at[0], or_s, mate).wait_recv()


def solution(mesh):
    def local(x, w, dy):
        rows, feats = x.shape
        half, cols = w.shape
        steps = rows // T
        any_ = pl.BlockSpec(memory_space=pl.ANY)
        dma = pltpu.SemaphoreType.DMA
        res = pl.pallas_call(
            kernel,
            out_shape=[
                jax.ShapeDtypeStruct((rows, feats), jnp.bfloat16),
                jax.ShapeDtypeStruct((half, cols), jnp.float32),
                jax.ShapeDtypeStruct((rows, cols), jnp.bfloat16),
                jax.ShapeDtypeStruct((rows, cols), jnp.bfloat16),
                jax.ShapeDtypeStruct((rows, cols), jnp.bfloat16),
            ],
            in_specs=[any_] * 3,
            out_specs=[any_, pl.BlockSpec(memory_space=pltpu.VMEM), any_, any_, any_],
            scratch_shapes=[
                pltpu.VMEM((half, cols), jnp.bfloat16),
                pltpu.VMEM((4 * rows, half), jnp.bfloat16),
                pltpu.VMEM((2 * T, cols), jnp.bfloat16),
                pltpu.VMEM((half, 2 * T), jnp.bfloat16),
                pltpu.VMEM((2 * steps, 2 * T, half), jnp.float32),
                pltpu.VMEM((2 * steps, 2 * T, half), jnp.float32),
                pltpu.VMEM((2 * steps, 2 * T, half), jnp.bfloat16),
                dma((2,)), dma, dma, dma((3,)), dma((4,)), dma((2,)),
                dma, dma((steps,)), dma, dma((steps,)), dma, dma((steps,)),
                dma, dma((2 * steps,)), dma((3,)), dma, dma,
            ],
            compiler_params=pltpu.CompilerParams(collective_id=0, has_side_effects=True,
                                                 vmem_limit_bytes=60 * 1024 * 1024),
        )(x, w, dy)
        return res[0], res[1]

    act = P(("dp", "r"), "c")
    return jax.shard_map(local, mesh=mesh, in_specs=(act, P("r", "c"), act),
                         out_specs=(act, act), check_vma=False)
```

```python
import jax
import jax.numpy as jnp
from jax import lax
from jax.experimental import pallas as pl
from jax.experimental.pallas import tpu as pltpu
from jax.sharding import PartitionSpec as P

MESH = pl.DeviceIdType.MESH
T = 64
TILE = 1024


def kernel(x, w, dy, dx, dw, far, far2, near, wv, xg, buf, xt, part, part_in, out,
           load_s, w_s, xl_s, xs_s, xr_s, xf_s, ys_s, yr_s, ns_s, nr_s, fs_s, fr_s,
           ps_s, pr_s, os_s, or_s, ol_s):
    rows, half = x.shape[0], x.shape[1] // 2
    cols = w.shape[1]
    steps = rows // T
    z, c, r = lax.axis_index("dp"), lax.axis_index("c"), lax.axis_index("r")
    chip, core = r // 2, r % 2
    far_chip = 1 - chip
    here = chip == c

    def device(cc, chip_, core_):
        return {"dp": z, "c": cc, "r": 2 * chip_ + core_}

    mate = device(c, chip, 1 - core)
    x_same, x_other = device(c, far_chip, core), device(c, far_chip, 1 - core)
    y_same, y_other = device(1 - c, chip, core), device(1 - c, chip, 1 - core)

    def remote(src, dst, send, recv, dev):
        return pltpu.make_async_remote_copy(src, dst, send, recv, device_id=dev,
                                            device_id_type=MESH)

    def x_block(t):
        return xg.at[pl.ds(pl.multiple_of(t * rows, rows), rows), :]

    def x_half(k):
        return x.at[:, pl.ds(pl.multiple_of(k * half, half), half)]

    def piece(ref, q):
        return ref.at[pl.ds(pl.multiple_of(q * T, T), T), :]

    barrier = pltpu.get_barrier_semaphore()
    peers = (mate, x_same, x_other, y_same, y_other)
    for p in peers:
        pl.semaphore_signal(barrier, inc=1, device_id=p, device_id_type=MESH)
    pl.semaphore_wait(barrier, len(peers))

    @pl.when(jnp.logical_not(here))
    def _():
        remote(x_half(core), x_block(r), xs_s.at[0], xr_s.at[r], x_same).start()
        remote(x_half(1 - core), x_block(r), xs_s.at[1], xr_s.at[r], x_other).start()

    @pl.when(here)
    def _():
        remote(x_half(core), x_block(r), xs_s.at[0], xr_s.at[r], y_same).start()
        remote(x_half(1 - core), x_block(r), xs_s.at[1], xr_s.at[r], y_other).start()
        remote(x_half(1 - core), x_block(r), xs_s.at[2], xr_s.at[r], mate).start()
        pltpu.make_async_copy(x_half(core), x_block(r), xl_s).start()

    @pl.loop(0, steps)
    def _(q):
        remote(piece(dy, q), piece(far, q), ys_s, yr_s.at[q], x_same).start()

    @pl.loop(0, steps)
    def _(q):
        remote(piece(dy, q), piece(near, q), ns_s, nr_s.at[q], mate).start()

    pltpu.make_async_copy(w, wv, w_s).start()

    @pl.loop(0, cols // TILE)
    def _(t):
        dw[:, pl.ds(pl.multiple_of(t * TILE, TILE), TILE)] = jnp.zeros((dw.shape[0], TILE), jnp.float32)

    pltpu.make_async_copy(w, wv, w_s).wait()

    mine, other = r, 2 * chip + 1 - core
    far_mine, far_other = 2 * far_chip + core, 2 * far_chip + 1 - core

    @pl.when(here)
    def _():
        pltpu.make_async_copy(x_half(core), x_block(r), xl_s).wait()

    @pl.when(jnp.logical_not(here))
    def _():
        remote(x_half(core), x_block(mine), xs_s.at[0], xr_s.at[mine], y_same).wait_recv()

    remote(x_half(core), x_block(other), xs_s.at[0], xr_s.at[other], y_same).wait_recv()

    def compute(slot, ta, tb, q):
        row = pl.multiple_of(q * T, T)
        xa = xg[pl.ds(pl.multiple_of(ta * rows + row, T), T), :]
        xb = xg[pl.ds(pl.multiple_of(tb * rows + row, T), T), :]
        xt[...] = jnp.concatenate([xa, xb], axis=0).T
        part[slot] = jnp.zeros(part.shape[1:], jnp.float32)

        @pl.loop(0, cols // TILE)
        def _(t):
            cs = pl.ds(pl.multiple_of(t * TILE, TILE), TILE)
            d = buf[:, cs]
            part[slot] += lax.dot_general(d, wv[:, cs], (((1,), (1,)), ((), ())),
                                          preferred_element_type=jnp.float32)
            dw[:, cs] += jnp.dot(xt[...], d, preferred_element_type=jnp.float32)

    def load(src, q, lo):
        return pltpu.make_async_copy(piece(src, q), buf.at[pl.ds(lo * T, T), :], load_s.at[lo])

    def send_part(slot):
        return remote(part.at[slot], part_in.at[slot], ps_s, pr_s.at[slot], y_same)

    @pl.loop(0, steps)
    def _(q):
        load(dy, q, 0).start()
        remote(piece(dy, q), piece(near, q), ns_s, nr_s.at[q], mate).wait_recv()
        load(near, q, 1).start()
        load(dy, q, 0).wait()
        load(near, q, 1).wait()
        compute(q, mine, other, q)

        @pl.when(jnp.logical_not(here))
        def _():
            send_part(q).start()

    for t in range(2):
        src_t = 2 * far_chip + t
        remote(x_half(core), x_block(src_t), xs_s.at[0], xr_s.at[src_t], x_same).wait_recv()

        @pl.when(here)
        def _():
            remote(x_block(src_t), x_block(src_t), xf_s.at[t], xr_s.at[src_t], y_same).start()

    def dx_piece(q):
        return dx.at[pl.ds(pl.multiple_of(q * T, T), T),
                     pl.ds(pl.multiple_of(core * half, half), half)]

    def finish(slot):
        send_part(slot).wait_recv()
        out[slot] = (part[slot] + part_in[slot]).astype(jnp.bfloat16)

    @pl.loop(0, steps)
    def _(q):
        slot = steps + q
        remote(piece(dy, q), piece(far, q), ys_s, yr_s.at[q], x_same).wait_recv()
        remote(piece(far, q), piece(far2, q), fs_s, fr_s.at[q], mate).start()
        load(far, q, 0).start()
        remote(piece(far, q), piece(far2, q), fs_s, fr_s.at[q], mate).wait_recv()
        load(far2, q, 1).start()
        load(far, q, 0).wait()
        load(far2, q, 1).wait()
        compute(slot, far_mine, far_other, q)

        @pl.when(jnp.logical_not(here))
        def _():
            send_part(slot).start()

        @pl.when(here)
        def _():
            finish(slot)
            remote(out.at[slot, pl.ds(0, T), :], dx_piece(q), os_s.at[0], or_s, x_same).start()
            remote(out.at[slot, pl.ds(T, T), :], dx_piece(q), os_s.at[1], or_s, x_other).start()
            finish(q)
            dx[pl.ds(pl.multiple_of(q * T, T), T), pl.ds(pl.multiple_of(core * half, half), half)] = out[q, 0:T, :]
            remote(out.at[q, pl.ds(T, T), :], dx_piece(q), os_s.at[2], or_s, mate).start()

    remote(dy, far, ys_s, yr_s.at[0], x_same).wait_send()
    remote(dy, near, ns_s, nr_s.at[0], mate).wait_send()
    remote(far, far2, fs_s, fr_s.at[0], mate).wait_send()
    for t in range(2):
        remote(x_half(core), x_block(r), xs_s.at[t], xr_s.at[r], x_same).wait_send()

    @pl.when(jnp.logical_not(here))
    def _():
        remote(part, part_in, ps_s, pr_s.at[0], y_same).wait_send()
        remote(dx, dx, os_s.at[0], or_s, x_same).wait_recv()

    @pl.when(here)
    def _():
        remote(x_half(core), x_block(r), xs_s.at[2], xr_s.at[r], mate).wait_send()
        for t in range(2):
            remote(x_block(t), x_block(t), xf_s.at[t], xr_s.at[r], y_same).wait_send()
        dx_half = dx.at[:, pl.ds(0, half)]
        for t in range(3):
            remote(dx_half, dx_half, os_s.at[t], or_s, mate).wait_send()
        remote(dx_half, dx_half, os_s.at[0], or_s, mate).wait_recv()


def store(dx_in, dw_in, dx, dw, sem):
    n = 8
    copies = [pltpu.make_async_copy(dx_in, dx, sem.at[n])]
    step = dw.shape[0] // n
    for i in range(n):
        rs = pl.ds(i * step, step)
        copies.append(pltpu.make_async_copy(dw_in.at[rs, :], dw.at[rs, :], sem.at[i]))
    for cp in copies:
        cp.start()
    for cp in copies:
        cp.wait()


def solution(mesh):
    def local(x, w, dy):
        rows, feats = x.shape
        half, cols = w.shape
        steps = rows // T
        any_ = pl.BlockSpec(memory_space=pl.ANY)
        dma = pltpu.SemaphoreType.DMA
        res = pl.pallas_call(
            kernel,
            out_shape=[
                pltpu.VMEM((rows, feats), jnp.bfloat16),
                pltpu.VMEM((half, cols), jnp.float32),
                jax.ShapeDtypeStruct((rows, cols), jnp.bfloat16),
                jax.ShapeDtypeStruct((rows, cols), jnp.bfloat16),
                jax.ShapeDtypeStruct((rows, cols), jnp.bfloat16),
            ],
            in_specs=[any_] * 3,
            out_specs=[pl.BlockSpec(memory_space=pltpu.VMEM), pl.BlockSpec(memory_space=pltpu.VMEM), any_, any_, any_],
            scratch_shapes=[
                pltpu.VMEM((half, cols), jnp.bfloat16),
                pltpu.VMEM((4 * rows, half), jnp.bfloat16),
                pltpu.VMEM((2 * T, cols), jnp.bfloat16),
                pltpu.VMEM((half, 2 * T), jnp.bfloat16),
                pltpu.VMEM((2 * steps, 2 * T, half), jnp.float32),
                pltpu.VMEM((2 * steps, 2 * T, half), jnp.float32),
                pltpu.VMEM((2 * steps, 2 * T, half), jnp.bfloat16),
                dma((2,)), dma, dma, dma((3,)), dma((4,)), dma((2,)),
                dma, dma((steps,)), dma, dma((steps,)), dma, dma((steps,)),
                dma, dma((2 * steps,)), dma((3,)), dma, dma,
            ],
            compiler_params=pltpu.CompilerParams(collective_id=0, has_side_effects=True,
                                                 vmem_limit_bytes=40 * 1024 * 1024),
        )(x, w, dy)
        vmem = pl.BlockSpec(memory_space=pltpu.VMEM)
        return pl.pallas_call(
            store,
            out_shape=[jax.ShapeDtypeStruct((rows, feats), jnp.bfloat16),
                       jax.ShapeDtypeStruct((half, cols), jnp.float32)],
            in_specs=[vmem, vmem],
            out_specs=[any_, any_],
            scratch_shapes=[dma((9,))],
            compiler_params=pltpu.CompilerParams(vmem_limit_bytes=1024 * 1024),
        )(res[0], res[1])

    act = P(("dp", "r"), "c")
    return jax.shard_map(local, mesh=mesh, in_specs=(act, P("r", "c"), act),
                         out_specs=(act, act), check_vma=False)
```

```python
import jax
import jax.numpy as jnp
from jax import lax
from jax.experimental import pallas as pl
from jax.experimental.pallas import tpu as pltpu
from jax.sharding import PartitionSpec as P

MESH = pl.DeviceIdType.MESH
T = 64
TILE = 1024
G = 32
WIDE = 2048


def kernel(x, w, dy, dx, dw, far, far2, near, wt, xg, buf, xt, last, part, part_in, out,
           load_s, w_s, xl_s, xs_s, xr_s, xf_s, ys_s, yr_s, ns_s, nr_s, fs_s, fr_s,
           ts_s, tr_s, us_s, ur_s, ps_s, pr_s, os_s, or_s):
    rows, half = x.shape[0], x.shape[1] // 2
    cols = w.shape[1]
    steps = rows // T
    main = steps - 1
    wide = cols // WIDE
    z, c, r = lax.axis_index("dp"), lax.axis_index("c"), lax.axis_index("r")
    chip, core = r // 2, r % 2
    far_chip = 1 - chip
    here = chip == c

    def device(cc, chip_, core_):
        return {"dp": z, "c": cc, "r": 2 * chip_ + core_}

    mate = device(c, chip, 1 - core)
    x_same, x_other = device(c, far_chip, core), device(c, far_chip, 1 - core)
    y_same, y_other = device(1 - c, chip, core), device(1 - c, chip, 1 - core)

    def remote(src, dst, send, recv, dev):
        return pltpu.make_async_remote_copy(src, dst, send, recv, device_id=dev,
                                            device_id_type=MESH)

    def x_block(t):
        return xg.at[pl.ds(pl.multiple_of(t * rows, rows), rows), :]

    def x_half(k):
        return x.at[:, pl.ds(pl.multiple_of(k * half, half), half)]

    def piece(ref, q):
        return ref.at[pl.ds(pl.multiple_of(q * T, T), T), :]

    barrier = pltpu.get_barrier_semaphore()
    peers = (mate, x_same, x_other, y_same, y_other)
    for p in peers:
        pl.semaphore_signal(barrier, inc=1, device_id=p, device_id_type=MESH)
    pl.semaphore_wait(barrier, len(peers))

    @pl.when(jnp.logical_not(here))
    def _():
        remote(x_half(core), x_block(r), xs_s.at[0], xr_s.at[r], x_same).start()
        remote(x_half(1 - core), x_block(r), xs_s.at[1], xr_s.at[r], x_other).start()

    @pl.when(here)
    def _():
        remote(x_half(core), x_block(r), xs_s.at[0], xr_s.at[r], y_same).start()
        remote(x_half(1 - core), x_block(r), xs_s.at[1], xr_s.at[r], y_other).start()
        remote(x_half(1 - core), x_block(r), xs_s.at[2], xr_s.at[r], mate).start()
        pltpu.make_async_copy(x_half(core), x_block(r), xl_s).start()

    @pl.loop(0, main)
    def _(q):
        remote(piece(dy, q), piece(far, q), ys_s, yr_s.at[q], x_same).start()

    def wide_cols(p):
        return pl.ds(pl.multiple_of(p * WIDE, WIDE), WIDE)

    def send_last(g, p):
        row = pl.multiple_of(main * T + g * G, G)
        return remote(dy.at[pl.ds(row, G), wide_cols(p)], last.at[g, pl.ds(0, G), wide_cols(p)],
                      ts_s, tr_s.at[g, p], x_same)

    def pass_last(g, p):
        return remote(last.at[g, pl.ds(0, G), wide_cols(p)], last.at[g, pl.ds(G, G), wide_cols(p)],
                      us_s, ur_s.at[g, p], mate)

    for g in range(2):
        @pl.loop(0, wide)
        def _(p):
            send_last(g, p).start()

    @pl.loop(0, steps)
    def _(q):
        remote(piece(dy, q), piece(near, q), ns_s, nr_s.at[q], mate).start()

    @pl.loop(0, cols // TILE)
    def _(t):
        dw[:, pl.ds(pl.multiple_of(t * TILE, TILE), TILE)] = jnp.zeros((dw.shape[0], TILE), jnp.float32)

    for b in range(w.shape[0] // (2 * T)):
        cp = pltpu.make_async_copy(w.at[pl.ds(b * 2 * T, 2 * T), :], buf, w_s)
        cp.start()
        cp.wait()

        @pl.loop(0, cols // TILE)
        def _(t):
            cs = pl.ds(pl.multiple_of(t * TILE, TILE), TILE)
            wt[cs, b * 2 * T:(b + 1) * 2 * T] = buf[:, cs].T

    mine, other = r, 2 * chip + 1 - core
    far_mine, far_other = 2 * far_chip + core, 2 * far_chip + 1 - core

    @pl.when(here)
    def _():
        pltpu.make_async_copy(x_half(core), x_block(r), xl_s).wait()

    @pl.when(jnp.logical_not(here))
    def _():
        remote(x_half(core), x_block(mine), xs_s.at[0], xr_s.at[mine], y_same).wait_recv()

    remote(x_half(core), x_block(other), xs_s.at[0], xr_s.at[other], y_same).wait_recv()

    def compute(slot, ta, tb, q):
        row = pl.multiple_of(q * T, T)
        xa = xg[pl.ds(pl.multiple_of(ta * rows + row, T), T), :]
        xb = xg[pl.ds(pl.multiple_of(tb * rows + row, T), T), :]
        xt[...] = jnp.concatenate([xa, xb], axis=0).T
        part[slot] = jnp.zeros(part.shape[1:], jnp.float32)

        @pl.loop(0, cols // TILE)
        def _(t):
            cs = pl.ds(pl.multiple_of(t * TILE, TILE), TILE)
            d = buf[:, cs]
            part[slot] += jnp.dot(d, wt[cs, :], preferred_element_type=jnp.float32)
            dw[:, cs] += jnp.dot(xt[...], d, preferred_element_type=jnp.float32)

    def load(src, q, lo):
        return pltpu.make_async_copy(piece(src, q), buf.at[pl.ds(lo * T, T), :], load_s.at[lo])

    def send_part(slot):
        return remote(part.at[slot], part_in.at[slot], ps_s, pr_s.at[slot], y_same)

    @pl.loop(0, steps)
    def _(q):
        load(dy, q, 0).start()
        remote(piece(dy, q), piece(near, q), ns_s, nr_s.at[q], mate).wait_recv()
        load(near, q, 1).start()
        load(dy, q, 0).wait()
        load(near, q, 1).wait()
        compute(q, mine, other, q)

        @pl.when(jnp.logical_not(here))
        def _():
            send_part(q).start()

    for t in range(2):
        src_t = 2 * far_chip + t
        remote(x_half(core), x_block(src_t), xs_s.at[0], xr_s.at[src_t], x_same).wait_recv()

        @pl.when(here)
        def _():
            remote(x_block(src_t), x_block(src_t), xf_s.at[t], xr_s.at[src_t], y_same).start()

    def dx_piece(q):
        return dx.at[pl.ds(pl.multiple_of(q * T, T), T),
                     pl.ds(pl.multiple_of(core * half, half), half)]

    def finish_near(q):
        send_part(q).wait_recv()
        out[q] = (part[q] + part_in[q]).astype(jnp.bfloat16)
        dx[pl.ds(pl.multiple_of(q * T, T), T),
           pl.ds(pl.multiple_of(core * half, half), half)] = out[q, 0:T, :]
        remote(out.at[q, pl.ds(T, T), :], dx_piece(q), os_s.at[2], or_s, mate).start()

    @pl.loop(0, main)
    def _(q):
        slot = steps + q
        remote(piece(dy, q), piece(far, q), ys_s, yr_s.at[q], x_same).wait_recv()
        remote(piece(far, q), piece(far2, q), fs_s, fr_s.at[q], mate).start()
        load(far, q, 0).start()
        remote(piece(far, q), piece(far2, q), fs_s, fr_s.at[q], mate).wait_recv()
        load(far2, q, 1).start()
        load(far, q, 0).wait()
        load(far2, q, 1).wait()
        compute(slot, far_mine, far_other, q)

        @pl.when(jnp.logical_not(here))
        def _():
            send_part(slot).start()

        @pl.when(here)
        def _():
            send_part(slot).wait_recv()
            out[slot] = (part[slot] + part_in[slot]).astype(jnp.bfloat16)
            remote(out.at[slot, pl.ds(0, T), :], dx_piece(q), os_s.at[0], or_s, x_same).start()
            remote(out.at[slot, pl.ds(T, T), :], dx_piece(q), os_s.at[1], or_s, x_other).start()
            finish_near(q)

    @pl.when(here)
    def _():
        finish_near(main)

    slot = 2 * steps - 1
    part[slot] = jnp.zeros(part.shape[1:], jnp.float32)
    for g in range(2):
        row = main * T + g * G
        xa = xg[pl.ds(pl.multiple_of(far_mine * rows + row, G), G), :]
        xb = xg[pl.ds(pl.multiple_of(far_other * rows + row, G), G), :]
        xt[:, g * 2 * G:(g + 1) * 2 * G] = jnp.concatenate([xa, xb], axis=0).T

    def arrive(g, p):
        send_last(g, p).wait_recv()
        pass_last(g, p).start()

    def products(g, p):
        pass_last(g, p).wait_recv()
        cs = wide_cols(p)
        part[slot, g * 2 * G:(g + 1) * 2 * G, :] += jnp.dot(
            last[g, :, cs], wt[cs, :], preferred_element_type=jnp.float32)

    def weights(g, p):
        cs = wide_cols(p)
        dw[:, cs] += jnp.dot(xt[:, g * 2 * G:(g + 1) * 2 * G], last[g, :, cs],
                             preferred_element_type=jnp.float32)

    arrive(0, 0)
    for g in range(2):
        row = main * T + g * G
        group = pl.ds(g * 2 * G, 2 * G)

        def send_group():
            return remote(part.at[slot, group, :], part_in.at[slot, group, :], ps_s,
                          pr_s.at[slot + g], y_same)

        @pl.loop(0, wide - 1)
        def _(p):
            arrive(g, p + 1)
            products(g, p)
            weights(g, p)

        if g == 0:
            arrive(1, 0)
        products(g, wide - 1)

        @pl.when(jnp.logical_not(here))
        def _():
            send_group().start()

        @pl.when(here)
        def _():
            send_group().wait_recv()
            out[slot, group, :] = (part[slot, group, :] + part_in[slot, group, :]).astype(jnp.bfloat16)
            target = dx.at[pl.ds(row, G), pl.ds(pl.multiple_of(core * half, half), half)]
            for k, dev in ((0, x_same), (1, x_other)):
                remote(out.at[slot, pl.ds(g * 2 * G + k * G, G), :], target, os_s.at[k], or_s, dev).start()

        weights(g, wide - 1)

    first = pl.ds(0, main * T)
    remote(dy.at[first, :], far.at[first, :], ys_s, yr_s.at[0], x_same).wait_send()
    rest = dy.at[pl.ds(main * T, 2 * G), :]
    remote(rest, rest, ts_s, tr_s.at[0, 0], x_same).wait_send()
    remote(rest, rest, us_s, ur_s.at[0, 0], mate).wait_send()
    remote(dy, near, ns_s, nr_s.at[0], mate).wait_send()
    remote(far.at[first, :], far2.at[first, :], fs_s, fr_s.at[0], mate).wait_send()
    for t in range(2):
        remote(x_half(core), x_block(r), xs_s.at[t], xr_s.at[r], x_same).wait_send()

    @pl.when(jnp.logical_not(here))
    def _():
        remote(part, part_in, ps_s, pr_s.at[0], y_same).wait_send()
        remote(dx, dx, os_s.at[0], or_s, x_same).wait_recv()

    @pl.when(here)
    def _():
        remote(x_half(core), x_block(r), xs_s.at[2], xr_s.at[r], mate).wait_send()
        for t in range(2):
            remote(x_block(t), x_block(t), xf_s.at[t], xr_s.at[r], y_same).wait_send()
        dx_half = dx.at[:, pl.ds(0, half)]
        for t in range(3):
            remote(dx_half, dx_half, os_s.at[t], or_s, mate).wait_send()
        remote(dx_half, dx_half, os_s.at[0], or_s, mate).wait_recv()


def store(dx_in, dw_in, dx, dw, sem):
    n = 8
    copies = [pltpu.make_async_copy(dx_in, dx, sem.at[n])]
    step = dw.shape[0] // n
    for i in range(n):
        rs = pl.ds(i * step, step)
        copies.append(pltpu.make_async_copy(dw_in.at[rs, :], dw.at[rs, :], sem.at[i]))
    for cp in copies:
        cp.start()
    for cp in copies:
        cp.wait()


def solution(mesh):
    def local(x, w, dy):
        rows, feats = x.shape
        half, cols = w.shape
        steps = rows // T
        any_ = pl.BlockSpec(memory_space=pl.ANY)
        dma = pltpu.SemaphoreType.DMA
        res = pl.pallas_call(
            kernel,
            out_shape=[
                pltpu.VMEM((rows, feats), jnp.bfloat16),
                pltpu.VMEM((half, cols), jnp.float32),
                jax.ShapeDtypeStruct((rows, cols), jnp.bfloat16),
                jax.ShapeDtypeStruct((rows, cols), jnp.bfloat16),
                jax.ShapeDtypeStruct((rows, cols), jnp.bfloat16),
            ],
            in_specs=[any_] * 3,
            out_specs=[pl.BlockSpec(memory_space=pltpu.VMEM), pl.BlockSpec(memory_space=pltpu.VMEM), any_, any_, any_],
            scratch_shapes=[
                pltpu.VMEM((cols, half), jnp.bfloat16),
                pltpu.VMEM((4 * rows, half), jnp.bfloat16),
                pltpu.VMEM((2 * T, cols), jnp.bfloat16),
                pltpu.VMEM((half, 2 * T), jnp.bfloat16),
                pltpu.VMEM((2, 2 * G, cols), jnp.bfloat16),
                pltpu.VMEM((2 * steps, 2 * T, half), jnp.float32),
                pltpu.VMEM((2 * steps, 2 * T, half), jnp.float32),
                pltpu.VMEM((2 * steps, 2 * T, half), jnp.bfloat16),
                dma((2,)), dma, dma, dma((3,)), dma((4,)), dma((2,)),
                dma, dma((steps,)), dma, dma((steps,)), dma, dma((steps,)),
                dma, dma((2, cols // WIDE)), dma, dma((2, cols // WIDE)),
                dma, dma((2 * steps + 1,)), dma((3,)), dma,
            ],
            compiler_params=pltpu.CompilerParams(collective_id=0, has_side_effects=True,
                                                 vmem_limit_bytes=44 * 1024 * 1024),
        )(x, w, dy)
        vmem = pl.BlockSpec(memory_space=pltpu.VMEM)
        return pl.pallas_call(
            store,
            out_shape=[jax.ShapeDtypeStruct((rows, feats), jnp.bfloat16),
                       jax.ShapeDtypeStruct((half, cols), jnp.float32)],
            in_specs=[vmem, vmem],
            out_specs=[any_, any_],
            scratch_shapes=[dma((9,))],
            compiler_params=pltpu.CompilerParams(vmem_limit_bytes=1024 * 1024),
        )(res[0], res[1])

    act = P(("dp", "r"), "c")
    return jax.shard_map(local, mesh=mesh, in_specs=(act, P("r", "c"), act),
                         out_specs=(act, act), check_vma=False)
```

```python
import jax
import jax.numpy as jnp
from jax import lax
from jax.experimental import pallas as pl
from jax.experimental.pallas import tpu as pltpu
from jax.sharding import PartitionSpec as P

MESH = pl.DeviceIdType.MESH
T = 64
TILE = 1024
AHEAD = 3


def kernel(x, w, dy, dx, dw, far, far2, near, wt, xg, relay, buf, xt, part, part_in, out,
           load_s, w_s, xl_s, xs_s, xr_s, lo_s, hi_s, rel_s, ys_s, yr_s, ns_s, nr_s, fs_s, fr_s,
           ps_s, pr_s, os_s, or_s):
    rows, half = x.shape[0], x.shape[1] // 2
    cols = w.shape[1]
    steps = rows // T
    hr = rows // 2
    z, c, r = lax.axis_index("dp"), lax.axis_index("c"), lax.axis_index("r")
    chip, core = r // 2, r % 2
    far_chip = 1 - chip
    here = chip == c
    there = jnp.logical_not(here)

    def device(cc, chip_, core_):
        return {"dp": z, "c": cc, "r": 2 * chip_ + core_}

    mate = device(c, chip, 1 - core)
    x_same, x_other = device(c, far_chip, core), device(c, far_chip, 1 - core)
    y_same, y_other = device(1 - c, chip, core), device(1 - c, chip, 1 - core)
    d_same, d_other = device(1 - c, far_chip, core), device(1 - c, far_chip, 1 - core)

    def remote(src, dst, send, recv, dev):
        return pltpu.make_async_remote_copy(src, dst, send, recv, device_id=dev,
                                            device_id_type=MESH)

    def x_rows(t, lo, n):
        return xg.at[pl.ds(pl.multiple_of(t * rows + lo, hr), n), :]

    def x_block(t):
        return x_rows(t, 0, rows)

    def x_part(k, lo, n):
        return x.at[pl.ds(lo, n), pl.ds(pl.multiple_of(k * half, half), half)]

    def piece(ref, q):
        return ref.at[pl.ds(pl.multiple_of(q * T, T), T), :]

    mine, other = r, 2 * chip + 1 - core
    far_mine, far_other = 2 * far_chip + core, 2 * far_chip + 1 - core

    barrier = pltpu.get_barrier_semaphore()
    peers = (mate, x_same, x_other, y_same, y_other, d_same, d_other)
    for p in peers:
        pl.semaphore_signal(barrier, inc=1, device_id=p, device_id_type=MESH)
    pl.semaphore_wait(barrier, len(peers))

    @pl.when(there)
    def _():
        remote(x_part(core, 0, hr), x_rows(r, 0, hr), xs_s.at[0], lo_s.at[core], x_same).start()
        remote(x_part(1 - core, 0, hr), x_rows(r, 0, hr), xs_s.at[1], lo_s.at[core], x_other).start()
        remote(x_part(core, hr, hr), relay.at[core], xs_s.at[2], rel_s.at[core], y_same).start()
        remote(x_part(1 - core, hr, hr), relay.at[core], xs_s.at[3], rel_s.at[core], y_other).start()

    def send_dy(q):
        return remote(piece(dy, q), piece(far, q), ys_s, yr_s.at[q], x_same)

    @pl.loop(0, AHEAD)
    def _(q):
        send_dy(q).start()

    @pl.when(there)
    def _():
        @pl.loop(AHEAD, steps)
        def _(q):
            send_dy(q).start()

    @pl.when(here)
    def _():
        remote(x_part(core, 0, rows), x_block(r), xs_s.at[0], xr_s.at[core], y_same).start()
        remote(x_part(1 - core, 0, rows), x_block(r), xs_s.at[1], xr_s.at[core], y_other).start()
        remote(x_part(1 - core, 0, rows), x_block(r), xs_s.at[2], xr_s.at[core], mate).start()
        pltpu.make_async_copy(x_part(core, 0, rows), x_block(r), xl_s).start()

    @pl.loop(0, steps)
    def _(q):
        remote(piece(dy, q), piece(near, q), ns_s, nr_s.at[q], mate).start()

    @pl.loop(0, cols // TILE)
    def _(t):
        dw[:, pl.ds(pl.multiple_of(t * TILE, TILE), TILE)] = jnp.zeros((dw.shape[0], TILE), jnp.float32)

    for b in range(w.shape[0] // (2 * T)):
        cp = pltpu.make_async_copy(w.at[pl.ds(b * 2 * T, 2 * T), :], buf, w_s)
        cp.start()
        cp.wait()

        @pl.loop(0, cols // TILE)
        def _(t):
            cs = pl.ds(pl.multiple_of(t * TILE, TILE), TILE)
            wt[cs, b * 2 * T:(b + 1) * 2 * T] = buf[:, cs].T

    @pl.when(here)
    def _():
        for t in range(2):
            remote(relay.at[t], relay.at[t], xs_s.at[5 + t], rel_s.at[t], y_same).wait_recv()
            remote(relay.at[t], x_rows(2 * chip + t, hr, hr), xs_s.at[5 + t], hi_s.at[t], x_same).start()

        @pl.loop(AHEAD, steps)
        def _(q):
            send_dy(q).start()

    @pl.when(here)
    def _():
        pltpu.make_async_copy(x_part(core, 0, rows), x_block(r), xl_s).wait()

    @pl.when(there)
    def _():
        remote(x_block(mine), x_block(mine), xs_s.at[0], xr_s.at[core], y_same).wait_recv()

    remote(x_block(other), x_block(other), xs_s.at[0], xr_s.at[1 - core], y_same).wait_recv()

    def compute(slot, ta, tb, q):
        row = pl.multiple_of(q * T, T)
        xa = xg[pl.ds(pl.multiple_of(ta * rows + row, T), T), :]
        xb = xg[pl.ds(pl.multiple_of(tb * rows + row, T), T), :]
        xt[...] = jnp.concatenate([xa, xb], axis=0).T
        part[slot] = jnp.zeros(part.shape[1:], jnp.float32)

        @pl.loop(0, cols // TILE)
        def _(t):
            cs = pl.ds(pl.multiple_of(t * TILE, TILE), TILE)
            d = buf[:, cs]
            part[slot] += jnp.dot(d, wt[cs, :], preferred_element_type=jnp.float32)
            dw[:, cs] += jnp.dot(xt[...], d, preferred_element_type=jnp.float32)

    def load(src, q, lo):
        return pltpu.make_async_copy(piece(src, q), buf.at[pl.ds(lo * T, T), :], load_s.at[lo])

    def send_part(slot):
        return remote(part.at[slot], part_in.at[slot], ps_s, pr_s.at[slot], y_same)

    @pl.loop(0, steps)
    def _(q):
        load(dy, q, 0).start()
        remote(piece(dy, q), piece(near, q), ns_s, nr_s.at[q], mate).wait_recv()
        load(near, q, 1).start()
        load(dy, q, 0).wait()
        load(near, q, 1).wait()
        compute(q, mine, other, q)

        @pl.when(there)
        def _():
            send_part(q).start()

    def pass_x(t, lo, recv, dev):
        rows_t = x_rows(2 * far_chip + t, lo, hr)
        return remote(rows_t, rows_t, xs_s.at[7 + t], recv.at[t], dev)

    for t in range(2):
        pass_x(t, 0, lo_s, x_same).wait_recv()

        @pl.when(here)
        def _():
            pass_x(t, 0, lo_s, y_same).start()

    for t in range(2):
        pass_x(t, hr, hi_s, x_same).wait_recv()

        @pl.when(there)
        def _():
            pass_x(t, hr, hi_s, y_same).start()

    def dx_piece(q):
        return dx.at[pl.ds(pl.multiple_of(q * T, T), T),
                     pl.ds(pl.multiple_of(core * half, half), half)]

    def add(slot):
        send_part(slot).wait_recv()
        out[slot] = (part[slot] + part_in[slot]).astype(jnp.bfloat16)

    def finish_far(q, dev_a, dev_b):
        slot = steps + q
        add(slot)
        remote(out.at[slot, pl.ds(0, T), :], dx_piece(q), os_s.at[0], or_s, dev_a).start()
        remote(out.at[slot, pl.ds(T, T), :], dx_piece(q), os_s.at[1], or_s, dev_b).start()

    def finish(q):
        @pl.when(jnp.logical_and(here, q % 2 == 1))
        def _():
            finish_far(q, x_same, x_other)

        @pl.when(jnp.logical_and(there, q % 2 == 0))
        def _():
            finish_far(q, d_same, d_other)

    @pl.loop(0, steps)
    def _(q):
        slot = steps + q
        send_dy(q).wait_recv()
        remote(piece(far, q), piece(far2, q), fs_s, fr_s.at[q], mate).start()
        load(far, q, 0).start()
        remote(piece(far, q), piece(far2, q), fs_s, fr_s.at[q], mate).wait_recv()
        load(far2, q, 1).start()
        load(far, q, 0).wait()
        load(far2, q, 1).wait()
        compute(slot, far_mine, far_other, q)

        @pl.when(jnp.logical_or(jnp.logical_and(there, q % 2 == 1), jnp.logical_and(here, q % 2 == 0)))
        def _():
            send_part(slot).start()

        @pl.when(q > 0)
        def _():
            finish(q - 1)

        @pl.when(here)
        def _():
            add(q)
            dx[pl.ds(pl.multiple_of(q * T, T), T),
               pl.ds(pl.multiple_of(core * half, half), half)] = out[q, 0:T, :]
            remote(out.at[q, pl.ds(T, T), :], dx_piece(q), os_s.at[2], or_s, mate).start()

    finish(steps - 1)

    remote(dy, far, ys_s, yr_s.at[0], x_same).wait_send()
    remote(dy, near, ns_s, nr_s.at[0], mate).wait_send()
    remote(far, far2, fs_s, fr_s.at[0], mate).wait_send()
    dx_half = dx.at[:, pl.ds(0, half)]
    dx_quarter = dx.at[pl.ds(0, hr), pl.ds(0, half)]
    for t in range(2):
        remote(dx_quarter, dx_quarter, os_s.at[t], or_s, x_same).wait_send()

    @pl.when(there)
    def _():
        for t in range(4):
            remote(x_part(0, 0, hr), x_rows(r, 0, hr), xs_s.at[t], lo_s.at[0], x_same).wait_send()
        for t in range(2):
            pass_x(t, hr, hi_s, y_same).wait_send()
        some = part.at[pl.ds(0, steps + steps // 2)]
        remote(some, some, ps_s, pr_s.at[0], y_same).wait_send()
        remote(dx, dx, os_s.at[0], or_s, x_same).wait_recv()

    @pl.when(here)
    def _():
        for t in range(3):
            remote(x_part(0, 0, rows), x_block(r), xs_s.at[t], xr_s.at[0], y_same).wait_send()
        for t in range(2):
            remote(relay.at[t], relay.at[t], xs_s.at[5 + t], rel_s.at[t], x_same).wait_send()
            pass_x(t, 0, lo_s, y_same).wait_send()
        some = part.at[pl.ds(0, steps // 2)]
        remote(some, some, ps_s, pr_s.at[0], y_same).wait_send()
        remote(dx_half, dx_half, os_s.at[2], or_s, mate).wait_send()
        remote(dx_half, dx_half, os_s.at[0], or_s, mate).wait_recv()


def store(dx_in, dw_in, dx, dw, sem):
    n = 8
    copies = [pltpu.make_async_copy(dx_in, dx, sem.at[n])]
    step = dw.shape[0] // n
    for i in range(n):
        rs = pl.ds(i * step, step)
        copies.append(pltpu.make_async_copy(dw_in.at[rs, :], dw.at[rs, :], sem.at[i]))
    for cp in copies:
        cp.start()
    for cp in copies:
        cp.wait()


def solution(mesh):
    def local(x, w, dy):
        rows, feats = x.shape
        half, cols = w.shape
        steps = rows // T
        any_ = pl.BlockSpec(memory_space=pl.ANY)
        vmem = pl.BlockSpec(memory_space=pltpu.VMEM)
        dma = pltpu.SemaphoreType.DMA
        res = pl.pallas_call(
            kernel,
            out_shape=[
                pltpu.VMEM((rows, feats), jnp.bfloat16),
                pltpu.VMEM((half, cols), jnp.float32),
                jax.ShapeDtypeStruct((rows, cols), jnp.bfloat16),
                jax.ShapeDtypeStruct((rows, cols), jnp.bfloat16),
                jax.ShapeDtypeStruct((rows, cols), jnp.bfloat16),
            ],
            in_specs=[any_] * 3,
            out_specs=[vmem, vmem, any_, any_, any_],
            scratch_shapes=[
                pltpu.VMEM((cols, half), jnp.bfloat16),
                pltpu.VMEM((4 * rows, half), jnp.bfloat16),
                pltpu.VMEM((2, rows // 2, half), jnp.bfloat16),
                pltpu.VMEM((2 * T, cols), jnp.bfloat16),
                pltpu.VMEM((half, 2 * T), jnp.bfloat16),
                pltpu.VMEM((2 * steps, 2 * T, half), jnp.float32),
                pltpu.VMEM((2 * steps, 2 * T, half), jnp.float32),
                pltpu.VMEM((2 * steps, 2 * T, half), jnp.bfloat16),
                dma((2,)), dma, dma, dma((9,)), dma((2,)), dma((2,)), dma((2,)), dma((2,)),
                dma, dma((steps,)), dma, dma((steps,)), dma, dma((steps,)),
                dma, dma((2 * steps,)), dma((3,)), dma,
            ],
            compiler_params=pltpu.CompilerParams(collective_id=0, has_side_effects=True,
                                                 vmem_limit_bytes=44 * 1024 * 1024),
        )(x, w, dy)
        return pl.pallas_call(
            store,
            out_shape=[jax.ShapeDtypeStruct((rows, feats), jnp.bfloat16),
                       jax.ShapeDtypeStruct((half, cols), jnp.float32)],
            in_specs=[vmem, vmem],
            out_specs=[any_, any_],
            scratch_shapes=[dma((9,))],
            compiler_params=pltpu.CompilerParams(vmem_limit_bytes=1024 * 1024),
        )(res[0], res[1])

    act = P(("dp", "r"), "c")
    return jax.shard_map(local, mesh=mesh, in_specs=(act, P("r", "c"), act),
                         out_specs=(act, act), check_vma=False)
```

```python
import jax
import jax.numpy as jnp
from jax import lax
from jax.experimental import pallas as pl
from jax.experimental.pallas import tpu as pltpu
from jax.sharding import PartitionSpec as P

MESH = pl.DeviceIdType.MESH
T = 64
TILE = 1024
AHEAD = 3


def kernel(x, w, dy, dx, dw, far, far2, near, wt, xg, relay, buf, xt, part, part_in, out,
           load_s, w_s, xl_s, xs_s, xr_s, lo_s, hi_s, rel_s, ys_s, yr_s, ns_s, nr_s, fs_s, fr_s,
           ps_s, pr_s, os_s, or_s):
    rows, half = x.shape[0], x.shape[1] // 2
    cols = w.shape[1]
    steps = rows // T
    hr = rows // 2
    z, c, r = lax.axis_index("dp"), lax.axis_index("c"), lax.axis_index("r")
    chip, core = r // 2, r % 2
    far_chip = 1 - chip
    here = chip == c
    there = jnp.logical_not(here)

    def device(cc, chip_, core_):
        return {"dp": z, "c": cc, "r": 2 * chip_ + core_}

    mate = device(c, chip, 1 - core)
    x_same, x_other = device(c, far_chip, core), device(c, far_chip, 1 - core)
    y_same, y_other = device(1 - c, chip, core), device(1 - c, chip, 1 - core)
    d_same, d_other = device(1 - c, far_chip, core), device(1 - c, far_chip, 1 - core)

    def remote(src, dst, send, recv, dev):
        return pltpu.make_async_remote_copy(src, dst, send, recv, device_id=dev,
                                            device_id_type=MESH)

    def x_rows(t, lo, n):
        return xg.at[pl.ds(pl.multiple_of(t * rows + lo, hr), n), :]

    def x_block(t):
        return x_rows(t, 0, rows)

    def x_part(k, lo, n):
        return x.at[pl.ds(lo, n), pl.ds(pl.multiple_of(k * half, half), half)]

    def piece(ref, q):
        return ref.at[pl.ds(pl.multiple_of(q * T, T), T), :]

    mine, other = r, 2 * chip + 1 - core
    far_mine, far_other = 2 * far_chip + core, 2 * far_chip + 1 - core

    barrier = pltpu.get_barrier_semaphore()
    peers = (mate, x_same, x_other, y_same, y_other)
    for p in peers:
        pl.semaphore_signal(barrier, inc=1, device_id=p, device_id_type=MESH)

    @pl.when(there)
    def _():
        for p in (d_same, d_other):
            pl.semaphore_signal(barrier, inc=1, device_id=p, device_id_type=MESH)
        pl.semaphore_wait(barrier, len(peers) + 2)

    @pl.when(here)
    def _():
        pl.semaphore_wait(barrier, len(peers))

    @pl.when(there)
    def _():
        remote(x_part(core, 0, hr), x_rows(r, 0, hr), xs_s.at[0], lo_s.at[core], x_same).start()
        remote(x_part(1 - core, 0, hr), x_rows(r, 0, hr), xs_s.at[1], lo_s.at[core], x_other).start()
        remote(x_part(core, hr, hr), relay.at[core], xs_s.at[2], rel_s.at[core], y_same).start()
        remote(x_part(1 - core, hr, hr), relay.at[core], xs_s.at[3], rel_s.at[core], y_other).start()

    def send_dy(q):
        return remote(piece(dy, q), piece(far, q), ys_s, yr_s.at[q], x_same)

    @pl.loop(0, AHEAD)
    def _(q):
        send_dy(q).start()

    @pl.when(there)
    def _():
        @pl.loop(AHEAD, steps)
        def _(q):
            send_dy(q).start()

    @pl.when(here)
    def _():
        remote(x_part(core, 0, rows), x_block(r), xs_s.at[0], xr_s.at[core], y_same).start()
        remote(x_part(1 - core, 0, rows), x_block(r), xs_s.at[1], xr_s.at[core], y_other).start()
        remote(x_part(1 - core, 0, rows), x_block(r), xs_s.at[2], xr_s.at[core], mate).start()
        pltpu.make_async_copy(x_part(core, 0, rows), x_block(r), xl_s).start()

    @pl.loop(0, steps)
    def _(q):
        remote(piece(dy, q), piece(near, q), ns_s, nr_s.at[q], mate).start()

    for b in range(2):
        pltpu.make_async_copy(w.at[pl.ds(b * 2 * T, 2 * T), :], buf.at[b], w_s.at[b]).start()

    @pl.loop(0, cols // TILE)
    def _(t):
        dw[:, pl.ds(pl.multiple_of(t * TILE, TILE), TILE)] = jnp.zeros((dw.shape[0], TILE), jnp.float32)

    def load_w(b):
        return pltpu.make_async_copy(w.at[pl.ds(b * 2 * T, 2 * T), :], buf.at[b % 2], w_s.at[b % 2])

    blocks = w.shape[0] // (2 * T)
    for b in range(blocks):
        load_w(b).wait()

        @pl.loop(0, cols // TILE)
        def _(t):
            cs = pl.ds(pl.multiple_of(t * TILE, TILE), TILE)
            wt[cs, b * 2 * T:(b + 1) * 2 * T] = buf[b % 2, :, cs].T

        if b + 2 < blocks:
            load_w(b + 2).start()

    @pl.when(here)
    def _():
        for t in range(2):
            remote(relay.at[t], relay.at[t], xs_s.at[5 + t], rel_s.at[t], y_same).wait_recv()
            remote(relay.at[t], x_rows(2 * chip + t, hr, hr), xs_s.at[5 + t], hi_s.at[t], x_same).start()

        @pl.loop(AHEAD, steps)
        def _(q):
            send_dy(q).start()

    @pl.when(here)
    def _():
        pltpu.make_async_copy(x_part(core, 0, rows), x_block(r), xl_s).wait()

    @pl.when(there)
    def _():
        remote(x_block(mine), x_block(mine), xs_s.at[0], xr_s.at[core], y_same).wait_recv()

    remote(x_block(other), x_block(other), xs_s.at[0], xr_s.at[1 - core], y_same).wait_recv()

    def compute(slot, ta, tb, q):
        row = pl.multiple_of(q * T, T)
        xa = xg[pl.ds(pl.multiple_of(ta * rows + row, T), T), :]
        xb = xg[pl.ds(pl.multiple_of(tb * rows + row, T), T), :]
        xt[...] = jnp.concatenate([xa, xb], axis=0).T
        part[slot] = jnp.zeros(part.shape[1:], jnp.float32)

        @pl.loop(0, cols // TILE)
        def _(t):
            cs = pl.ds(pl.multiple_of(t * TILE, TILE), TILE)
            d = buf[q % 2, :, cs]
            part[slot] += jnp.dot(d, wt[cs, :], preferred_element_type=jnp.float32)
            dw[:, cs] += jnp.dot(xt[...], d, preferred_element_type=jnp.float32)

    def load(src, q, lo):
        return pltpu.make_async_copy(piece(src, q), buf.at[q % 2, pl.ds(lo * T, T), :], load_s.at[q % 2, lo])

    def send_part(slot):
        return remote(part.at[slot], part_in.at[slot], ps_s, pr_s.at[slot], y_same)

    def fetch_near(q):
        load(dy, q, 0).start()
        remote(piece(dy, q), piece(near, q), ns_s, nr_s.at[q], mate).wait_recv()
        load(near, q, 1).start()

    fetch_near(0)

    @pl.loop(0, steps)
    def _(q):
        @pl.when(q + 1 < steps)
        def _():
            fetch_near(q + 1)

        load(dy, q, 0).wait()
        load(near, q, 1).wait()
        compute(q, mine, other, q)

        @pl.when(there)
        def _():
            send_part(q).start()

    def pass_x(t, lo, recv, dev):
        rows_t = x_rows(2 * far_chip + t, lo, hr)
        return remote(rows_t, rows_t, xs_s.at[7 + t], recv.at[t], dev)

    for t in range(2):
        pass_x(t, 0, lo_s, x_same).wait_recv()

        @pl.when(here)
        def _():
            pass_x(t, 0, lo_s, y_same).start()

    for t in range(2):
        pass_x(t, hr, hi_s, x_same).wait_recv()

        @pl.when(there)
        def _():
            pass_x(t, hr, hi_s, y_same).start()

    def dx_piece(q):
        return dx.at[pl.ds(pl.multiple_of(q * T, T), T),
                     pl.ds(pl.multiple_of(core * half, half), half)]

    def add(slot):
        send_part(slot).wait_recv()
        out[slot] = (part[slot] + part_in[slot]).astype(jnp.bfloat16)

    def finish_far(q, dev_a, dev_b):
        slot = steps + q
        add(slot)
        remote(out.at[slot, pl.ds(0, T), :], dx_piece(q), os_s.at[0], or_s, dev_a).start()
        remote(out.at[slot, pl.ds(T, T), :], dx_piece(q), os_s.at[1], or_s, dev_b).start()

    def by_o(q):
        return jnp.logical_or(jnp.logical_and(q % 2 == 0, q < steps - 2), q == 1)

    def finish(q):
        @pl.when(jnp.logical_and(here, jnp.logical_not(by_o(q))))
        def _():
            finish_far(q, x_same, x_other)

        @pl.when(jnp.logical_and(there, by_o(q)))
        def _():
            finish_far(q, d_same, d_other)

    def work_far(q):
        slot = steps + q
        load(far, q, 0).wait()
        load(far2, q, 1).wait()
        compute(slot, far_mine, far_other, q)

        @pl.when(there != by_o(q))
        def _():
            send_part(slot).start()

        @pl.when(q > 0)
        def _():
            finish(q - 1)

        @pl.when(here)
        def _():
            add(q)
            dx[pl.ds(pl.multiple_of(q * T, T), T),
               pl.ds(pl.multiple_of(core * half, half), half)] = out[q, 0:T, :]
            remote(out.at[q, pl.ds(T, T), :], dx_piece(q), os_s.at[2], or_s, mate).start()

    @pl.loop(0, steps)
    def _(q):
        send_dy(q).wait_recv()
        load(far, q, 0).start()
        remote(piece(far, q), piece(far2, q), fs_s, fr_s.at[q], mate).start()
        remote(piece(far, q), piece(far2, q), fs_s, fr_s.at[q], mate).wait_recv()
        load(far2, q, 1).start()

        @pl.when(q > 0)
        def _():
            work_far(q - 1)

    work_far(jnp.int32(steps - 1))
    finish(steps - 1)

    remote(dy, far, ys_s, yr_s.at[0], x_same).wait_send()
    remote(dy, near, ns_s, nr_s.at[0], mate).wait_send()
    remote(far, far2, fs_s, fr_s.at[0], mate).wait_send()
    dx_half = dx.at[:, pl.ds(0, half)]
    dx_quarter = dx.at[pl.ds(0, hr), pl.ds(0, half)]
    for t in range(2):
        remote(dx_quarter, dx_quarter, os_s.at[t], or_s, x_same).wait_send()

    @pl.when(there)
    def _():
        for t in range(4):
            remote(x_part(0, 0, hr), x_rows(r, 0, hr), xs_s.at[t], lo_s.at[0], x_same).wait_send()
        for t in range(2):
            pass_x(t, hr, hi_s, y_same).wait_send()
        some = part.at[pl.ds(0, steps + steps // 2)]
        remote(some, some, ps_s, pr_s.at[0], y_same).wait_send()
        remote(dx, dx, os_s.at[0], or_s, x_same).wait_recv()

    @pl.when(here)
    def _():
        for t in range(3):
            remote(x_part(0, 0, rows), x_block(r), xs_s.at[t], xr_s.at[0], y_same).wait_send()
        for t in range(2):
            remote(relay.at[t], relay.at[t], xs_s.at[5 + t], rel_s.at[t], x_same).wait_send()
            pass_x(t, 0, lo_s, y_same).wait_send()
        some = part.at[pl.ds(0, steps // 2)]
        remote(some, some, ps_s, pr_s.at[0], y_same).wait_send()
        remote(dx_half, dx_half, os_s.at[2], or_s, mate).wait_send()
        remote(dx_half, dx_half, os_s.at[0], or_s, mate).wait_recv()


def store(dx_in, dw_in, dx, dw, sem):
    n = 8
    copies = [pltpu.make_async_copy(dx_in, dx, sem.at[n])]
    step = dw.shape[0] // n
    for i in range(n):
        rs = pl.ds(i * step, step)
        copies.append(pltpu.make_async_copy(dw_in.at[rs, :], dw.at[rs, :], sem.at[i]))
    for cp in copies:
        cp.start()
    for cp in copies:
        cp.wait()


def solution(mesh):
    def local(x, w, dy):
        rows, feats = x.shape
        half, cols = w.shape
        steps = rows // T
        any_ = pl.BlockSpec(memory_space=pl.ANY)
        vmem = pl.BlockSpec(memory_space=pltpu.VMEM)
        dma = pltpu.SemaphoreType.DMA
        res = pl.pallas_call(
            kernel,
            out_shape=[
                pltpu.VMEM((rows, feats), jnp.bfloat16),
                pltpu.VMEM((half, cols), jnp.float32),
                jax.ShapeDtypeStruct((rows, cols), jnp.bfloat16),
                jax.ShapeDtypeStruct((rows, cols), jnp.bfloat16),
                jax.ShapeDtypeStruct((rows, cols), jnp.bfloat16),
            ],
            in_specs=[any_] * 3,
            out_specs=[vmem, vmem, any_, any_, any_],
            scratch_shapes=[
                pltpu.VMEM((cols, half), jnp.bfloat16),
                pltpu.VMEM((4 * rows, half), jnp.bfloat16),
                pltpu.VMEM((2, rows // 2, half), jnp.bfloat16),
                pltpu.VMEM((2, 2 * T, cols), jnp.bfloat16),
                pltpu.VMEM((half, 2 * T), jnp.bfloat16),
                pltpu.VMEM((2 * steps, 2 * T, half), jnp.float32),
                pltpu.VMEM((2 * steps, 2 * T, half), jnp.float32),
                pltpu.VMEM((2 * steps, 2 * T, half), jnp.bfloat16),
                dma((2, 2)), dma((2,)), dma, dma((9,)), dma((2,)), dma((2,)), dma((2,)), dma((2,)),
                dma, dma((steps,)), dma, dma((steps,)), dma, dma((steps,)),
                dma, dma((2 * steps,)), dma((3,)), dma,
            ],
            compiler_params=pltpu.CompilerParams(collective_id=0, has_side_effects=True,
                                                 vmem_limit_bytes=44 * 1024 * 1024),
        )(x, w, dy)
        return pl.pallas_call(
            store,
            out_shape=[jax.ShapeDtypeStruct((rows, feats), jnp.bfloat16),
                       jax.ShapeDtypeStruct((half, cols), jnp.float32)],
            in_specs=[vmem, vmem],
            out_specs=[any_, any_],
            scratch_shapes=[dma((9,))],
            compiler_params=pltpu.CompilerParams(vmem_limit_bytes=1024 * 1024),
        )(res[0], res[1])

    act = P(("dp", "r"), "c")
    return jax.shard_map(local, mesh=mesh, in_specs=(act, P("r", "c"), act),
                         out_specs=(act, act), check_vma=False)
```

```python
import jax
import jax.numpy as jnp
from jax import lax
from jax.experimental import pallas as pl
from jax.experimental.pallas import tpu as pltpu
from jax.sharding import PartitionSpec as P

MESH = pl.DeviceIdType.MESH
T = 64
TILE = 1024
AHEAD = 3
LAST = 2


def kernel(x, w, dy, dx, dw, far, far2, near, wt, xg, relay, buf, xt, part, part_in, out,
           load_s, w_s, xl_s, xs_s, xr_s, lo_s, hi_s, rel_s, ys_s, yr_s, ns_s, nr_s, fs_s, fr_s,
           ts_s, tr_s, us_s, ur_s, ps_s, pr_s, os_s, or_s):
    rows, half = x.shape[0], x.shape[1] // 2
    cols = w.shape[1]
    steps = rows // T
    main = steps - LAST
    hr = rows // 2
    z, c, r = lax.axis_index("dp"), lax.axis_index("c"), lax.axis_index("r")
    chip, core = r // 2, r % 2
    far_chip = 1 - chip
    here = chip == c
    there = jnp.logical_not(here)

    def device(cc, chip_, core_):
        return {"dp": z, "c": cc, "r": 2 * chip_ + core_}

    mate = device(c, chip, 1 - core)
    x_same, x_other = device(c, far_chip, core), device(c, far_chip, 1 - core)
    y_same, y_other = device(1 - c, chip, core), device(1 - c, chip, 1 - core)
    d_same, d_other = device(1 - c, far_chip, core), device(1 - c, far_chip, 1 - core)

    def remote(src, dst, send, recv, dev):
        return pltpu.make_async_remote_copy(src, dst, send, recv, device_id=dev,
                                            device_id_type=MESH)

    def x_rows(t, lo, n):
        return xg.at[pl.ds(pl.multiple_of(t * rows + lo, hr), n), :]

    def x_block(t):
        return x_rows(t, 0, rows)

    def x_part(k, lo, n):
        return x.at[pl.ds(lo, n), pl.ds(pl.multiple_of(k * half, half), half)]

    def piece(ref, q):
        return ref.at[pl.ds(pl.multiple_of(q * T, T), T), :]

    mine, other = r, 2 * chip + 1 - core
    far_mine, far_other = 2 * far_chip + core, 2 * far_chip + 1 - core

    barrier = pltpu.get_barrier_semaphore()
    peers = (mate, x_same, x_other, y_same, y_other)
    for p in peers:
        pl.semaphore_signal(barrier, inc=1, device_id=p, device_id_type=MESH)

    @pl.when(there)
    def _():
        for p in (d_same, d_other):
            pl.semaphore_signal(barrier, inc=1, device_id=p, device_id_type=MESH)
        pl.semaphore_wait(barrier, len(peers) + 2)

    @pl.when(here)
    def _():
        pl.semaphore_wait(barrier, len(peers))

    @pl.when(there)
    def _():
        remote(x_part(core, 0, hr), x_rows(r, 0, hr), xs_s.at[0], lo_s.at[core], x_same).start()
        remote(x_part(1 - core, 0, hr), x_rows(r, 0, hr), xs_s.at[1], lo_s.at[core], x_other).start()
        remote(x_part(core, hr, hr), relay.at[core], xs_s.at[2], rel_s.at[core], y_same).start()
        remote(x_part(1 - core, hr, hr), relay.at[core], xs_s.at[3], rel_s.at[core], y_other).start()

    def send_dy(q):
        return remote(piece(dy, q), piece(far, q), ys_s, yr_s.at[q], x_same)

    def send_last(g):
        return remote(piece(dy, main + g), buf.at[2 + g, pl.ds(0, T), :], ts_s, tr_s.at[g], x_same)

    def pass_last(g):
        return remote(buf.at[2 + g, pl.ds(0, T), :], buf.at[2 + g, pl.ds(T, T), :], us_s, ur_s.at[g], mate)

    def send_rest():
        @pl.loop(AHEAD, main)
        def _(q):
            send_dy(q).start()

        for g in range(LAST):
            send_last(g).start()

    @pl.loop(0, AHEAD)
    def _(q):
        send_dy(q).start()

    @pl.when(there)
    def _():
        send_rest()

    @pl.when(here)
    def _():
        remote(x_part(core, 0, rows), x_block(r), xs_s.at[0], xr_s.at[core], y_same).start()
        remote(x_part(1 - core, 0, rows), x_block(r), xs_s.at[1], xr_s.at[core], y_other).start()
        remote(x_part(1 - core, 0, rows), x_block(r), xs_s.at[2], xr_s.at[core], mate).start()
        pltpu.make_async_copy(x_part(core, 0, rows), x_block(r), xl_s).start()

    @pl.loop(0, steps)
    def _(q):
        remote(piece(dy, q), piece(near, q), ns_s, nr_s.at[q], mate).start()

    for b in range(2):
        pltpu.make_async_copy(w.at[pl.ds(b * 2 * T, 2 * T), :], buf.at[b], w_s.at[b]).start()

    @pl.loop(0, cols // TILE)
    def _(t):
        dw[:, pl.ds(pl.multiple_of(t * TILE, TILE), TILE)] = jnp.zeros((dw.shape[0], TILE), jnp.float32)

    def load_w(b):
        return pltpu.make_async_copy(w.at[pl.ds(b * 2 * T, 2 * T), :], buf.at[b % 2], w_s.at[b % 2])

    blocks = w.shape[0] // (2 * T)
    for b in range(blocks):
        load_w(b).wait()

        @pl.loop(0, cols // TILE)
        def _(t):
            cs = pl.ds(pl.multiple_of(t * TILE, TILE), TILE)
            wt[cs, b * 2 * T:(b + 1) * 2 * T] = buf[b % 2, :, cs].T

        if b + 2 < blocks:
            load_w(b + 2).start()

    @pl.when(here)
    def _():
        for t in range(2):
            remote(relay.at[t], relay.at[t], xs_s.at[5 + t], rel_s.at[t], y_same).wait_recv()
            remote(relay.at[t], x_rows(2 * chip + t, hr, hr), xs_s.at[5 + t], hi_s.at[t], x_same).start()

        send_rest()

    @pl.when(here)
    def _():
        pltpu.make_async_copy(x_part(core, 0, rows), x_block(r), xl_s).wait()

    @pl.when(there)
    def _():
        remote(x_block(mine), x_block(mine), xs_s.at[0], xr_s.at[core], y_same).wait_recv()

    remote(x_block(other), x_block(other), xs_s.at[0], xr_s.at[1 - core], y_same).wait_recv()

    def compute(slot, ta, tb, q, b):
        row = pl.multiple_of(q * T, T)
        xa = xg[pl.ds(pl.multiple_of(ta * rows + row, T), T), :]
        xb = xg[pl.ds(pl.multiple_of(tb * rows + row, T), T), :]
        xt[...] = jnp.concatenate([xa, xb], axis=0).T
        part[slot] = jnp.zeros(part.shape[1:], jnp.float32)

        @pl.loop(0, cols // TILE)
        def _(t):
            cs = pl.ds(pl.multiple_of(t * TILE, TILE), TILE)
            d = buf[b, :, cs]
            part[slot] += jnp.dot(d, wt[cs, :], preferred_element_type=jnp.float32)
            dw[:, cs] += jnp.dot(xt[...], d, preferred_element_type=jnp.float32)

    def load(src, q, lo):
        return pltpu.make_async_copy(piece(src, q), buf.at[q % 2, pl.ds(lo * T, T), :], load_s.at[q % 2, lo])

    def send_part(slot):
        return remote(part.at[slot], part_in.at[slot], ps_s, pr_s.at[slot], y_same)

    def fetch_near(q):
        load(dy, q, 0).start()
        remote(piece(dy, q), piece(near, q), ns_s, nr_s.at[q], mate).wait_recv()
        load(near, q, 1).start()

    fetch_near(0)

    @pl.loop(0, steps)
    def _(q):
        @pl.when(q + 1 < steps)
        def _():
            fetch_near(q + 1)

        load(dy, q, 0).wait()
        load(near, q, 1).wait()
        compute(q, mine, other, q, q % 2)

        @pl.when(there)
        def _():
            send_part(q).start()

    def pass_x(t, lo, recv, dev):
        rows_t = x_rows(2 * far_chip + t, lo, hr)
        return remote(rows_t, rows_t, xs_s.at[7 + t], recv.at[t], dev)

    for t in range(2):
        pass_x(t, 0, lo_s, x_same).wait_recv()

        @pl.when(here)
        def _():
            pass_x(t, 0, lo_s, y_same).start()

    for t in range(2):
        pass_x(t, hr, hi_s, x_same).wait_recv()

        @pl.when(there)
        def _():
            pass_x(t, hr, hi_s, y_same).start()

    def dx_piece(q):
        return dx.at[pl.ds(pl.multiple_of(q * T, T), T),
                     pl.ds(pl.multiple_of(core * half, half), half)]

    def add(slot):
        send_part(slot).wait_recv()
        out[slot] = (part[slot] + part_in[slot]).astype(jnp.bfloat16)

    def finish_far(q, dev_a, dev_b):
        slot = steps + q
        add(slot)
        remote(out.at[slot, pl.ds(0, T), :], dx_piece(q), os_s.at[0], or_s, dev_a).start()
        remote(out.at[slot, pl.ds(T, T), :], dx_piece(q), os_s.at[1], or_s, dev_b).start()

    def by_o(q):
        return q % 2 == 0

    def finish(q):
        @pl.when(jnp.logical_and(here, jnp.logical_not(by_o(q))))
        def _():
            finish_far(q, x_same, x_other)

        @pl.when(jnp.logical_and(there, by_o(q)))
        def _():
            finish_far(q, d_same, d_other)

    def work_far(q, b):
        slot = steps + q
        compute(slot, far_mine, far_other, q, b)

        @pl.when(there != by_o(q))
        def _():
            send_part(slot).start()

        @pl.when(q > 0)
        def _():
            finish(q - 1)

        @pl.when(here)
        def _():
            add(q)
            dx[pl.ds(pl.multiple_of(q * T, T), T),
               pl.ds(pl.multiple_of(core * half, half), half)] = out[q, 0:T, :]
            remote(out.at[q, pl.ds(T, T), :], dx_piece(q), os_s.at[2], or_s, mate).start()

    def work_loaded(q):
        load(far, q, 0).wait()
        load(far2, q, 1).wait()
        work_far(q, q % 2)

    @pl.loop(0, main)
    def _(q):
        send_dy(q).wait_recv()
        load(far, q, 0).start()
        remote(piece(far, q), piece(far2, q), fs_s, fr_s.at[q], mate).start()
        remote(piece(far, q), piece(far2, q), fs_s, fr_s.at[q], mate).wait_recv()
        load(far2, q, 1).start()

        @pl.when(q > 0)
        def _():
            work_loaded(q - 1)

    work_loaded(jnp.int32(main - 1))
    for g in range(LAST):
        send_last(g).wait_recv()
        pass_last(g).start()
        pass_last(g).wait_recv()
        work_far(jnp.int32(main + g), 2 + g)

    finish(jnp.int32(steps - 1))

    first = pl.ds(0, main * T)
    rest = dy.at[pl.ds(main * T, LAST * T), :]
    remote(dy.at[first, :], far.at[first, :], ys_s, yr_s.at[0], x_same).wait_send()
    remote(rest, rest, ts_s, tr_s.at[0], x_same).wait_send()
    remote(rest, rest, us_s, ur_s.at[0], mate).wait_send()
    remote(dy, near, ns_s, nr_s.at[0], mate).wait_send()
    remote(far.at[first, :], far2.at[first, :], fs_s, fr_s.at[0], mate).wait_send()
    dx_half = dx.at[:, pl.ds(0, half)]
    dx_quarter = dx.at[pl.ds(0, hr), pl.ds(0, half)]
    for t in range(2):
        remote(dx_quarter, dx_quarter, os_s.at[t], or_s, x_same).wait_send()

    @pl.when(there)
    def _():
        for t in range(4):
            remote(x_part(0, 0, hr), x_rows(r, 0, hr), xs_s.at[t], lo_s.at[0], x_same).wait_send()
        for t in range(2):
            pass_x(t, hr, hi_s, y_same).wait_send()
        some = part.at[pl.ds(0, steps + steps // 2)]
        remote(some, some, ps_s, pr_s.at[0], y_same).wait_send()
        remote(dx, dx, os_s.at[0], or_s, x_same).wait_recv()

    @pl.when(here)
    def _():
        for t in range(3):
            remote(x_part(0, 0, rows), x_block(r), xs_s.at[t], xr_s.at[0], y_same).wait_send()
        for t in range(2):
            remote(relay.at[t], relay.at[t], xs_s.at[5 + t], rel_s.at[t], x_same).wait_send()
            pass_x(t, 0, lo_s, y_same).wait_send()
        some = part.at[pl.ds(0, steps // 2)]
        remote(some, some, ps_s, pr_s.at[0], y_same).wait_send()
        remote(dx_half, dx_half, os_s.at[2], or_s, mate).wait_send()
        remote(dx_half, dx_half, os_s.at[0], or_s, mate).wait_recv()


def store(dx_in, dw_in, dx, dw, sem):
    n = 8
    copies = [pltpu.make_async_copy(dx_in, dx, sem.at[n])]
    step = dw.shape[0] // n
    for i in range(n):
        rs = pl.ds(i * step, step)
        copies.append(pltpu.make_async_copy(dw_in.at[rs, :], dw.at[rs, :], sem.at[i]))
    for cp in copies:
        cp.start()
    for cp in copies:
        cp.wait()


def solution(mesh):
    def local(x, w, dy):
        rows, feats = x.shape
        half, cols = w.shape
        steps = rows // T
        any_ = pl.BlockSpec(memory_space=pl.ANY)
        vmem = pl.BlockSpec(memory_space=pltpu.VMEM)
        dma = pltpu.SemaphoreType.DMA
        res = pl.pallas_call(
            kernel,
            out_shape=[
                pltpu.VMEM((rows, feats), jnp.bfloat16),
                pltpu.VMEM((half, cols), jnp.float32),
                jax.ShapeDtypeStruct((rows, cols), jnp.bfloat16),
                jax.ShapeDtypeStruct((rows, cols), jnp.bfloat16),
                jax.ShapeDtypeStruct((rows, cols), jnp.bfloat16),
            ],
            in_specs=[any_] * 3,
            out_specs=[vmem, vmem, any_, any_, any_],
            scratch_shapes=[
                pltpu.VMEM((cols, half), jnp.bfloat16),
                pltpu.VMEM((4 * rows, half), jnp.bfloat16),
                pltpu.VMEM((2, rows // 2, half), jnp.bfloat16),
                pltpu.VMEM((2 + LAST, 2 * T, cols), jnp.bfloat16),
                pltpu.VMEM((half, 2 * T), jnp.bfloat16),
                pltpu.VMEM((2 * steps, 2 * T, half), jnp.float32),
                pltpu.VMEM((2 * steps, 2 * T, half), jnp.float32),
                pltpu.VMEM((2 * steps, 2 * T, half), jnp.bfloat16),
                dma((2, 2)), dma((2,)), dma, dma((9,)), dma((2,)), dma((2,)), dma((2,)), dma((2,)),
                dma, dma((steps,)), dma, dma((steps,)), dma, dma((steps,)),
                dma, dma((LAST,)), dma, dma((LAST,)),
                dma, dma((2 * steps,)), dma((3,)), dma,
            ],
            compiler_params=pltpu.CompilerParams(collective_id=0, has_side_effects=True,
                                                 vmem_limit_bytes=44 * 1024 * 1024),
        )(x, w, dy)
        return pl.pallas_call(
            store,
            out_shape=[jax.ShapeDtypeStruct((rows, feats), jnp.bfloat16),
                       jax.ShapeDtypeStruct((half, cols), jnp.float32)],
            in_specs=[vmem, vmem],
            out_specs=[any_, any_],
            scratch_shapes=[dma((9,))],
            compiler_params=pltpu.CompilerParams(vmem_limit_bytes=1024 * 1024),
        )(res[0], res[1])

    act = P(("dp", "r"), "c")
    return jax.shard_map(local, mesh=mesh, in_specs=(act, P("r", "c"), act),
                         out_specs=(act, act), check_vma=False)
```
